32 devices in a mesh: row: 4 (over x, core), col: 8 (over z, y).
Axes of the slice: x: 2, y: 2, z: 4, core: 2. Of those that a mesh axis runs over, the one named last changes fastest.
Arguments:
- panel_rows: float32 [4096, 4096], P('row', 'col'), may hold values from -0.75 to 0.75
- owner_slot: int32 [8, 8], replicated, may hold values from -1 to 15, as said below
Outputs:
- packed: float32 [4, 16, 512, 512], P('row', 'col')
The draws below stay inside these ranges and needn't reach their ends.
Inputs may be any that keep to these rules, and one draw needn't show every extreme that they name: For j <= i, owner_slot[i, j] is the position of tile (i, j) among the 16 positions of group i // 2; tiles of one group have distinct positions; entries above the diagonal are -1. Position p lies on the device of col index p // 2.
All inputs are finite; a program needn't handle non-finite values.
Results may differ from the reference program's by a relative error of at most 0.0003.
Values sent between devices are 32-bit elements; how exact they have to be, the bound alone decides.
A program may use at most 128 MiB of HBM per device.

```python
import jax
import jax.numpy as jnp
from jax import lax

BLOCK = 512
K = 4096
ORDER = 4096
BR = 2
NB = 8
POS = 16
N_ROW = 4


def draw_owner_slot(key, part):
    groups = NB // BR
    block_row = jnp.arange(NB, dtype=jnp.int32)[:, None]
    block_col = jnp.arange(NB, dtype=jnp.int32)[None, :]
    row_keys = jax.random.split(jax.random.fold_in(key, 11), groups)
    orders = jax.vmap(lambda sub_key: jax.random.permutation(sub_key, POS))(row_keys).astype(jnp.int32)
    group_ids = jnp.arange(groups, dtype=jnp.int32)
    first_rows = group_ids * BR
    tile_total = BR * first_rows + BR * (BR + 1) // 2
    picked = jax.random.randint(jax.random.fold_in(key, 12), (groups,), 0, tile_total).astype(jnp.int32)
    top_place = jnp.argmax(orders == POS - 1, axis=1).astype(jnp.int32)
    offsets = top_place - picked
    row_group = block_row // BR
    first_own = row_group * BR
    index_in = (block_row * (block_row + 1) - first_own * (first_own + 1)) // 2 + block_col
    taken = (index_in + offsets[row_group[:, 0]][:, None]) % POS
    order_rows = orders[row_group[:, 0]]
    placed = jnp.take_along_axis(order_rows, taken, axis=1)
    return jnp.where(block_col <= block_row, placed, -1).astype(jnp.int32)


def levels(stream_key, extent, cuts, low, largest):
    level, own = 1.0, jax.random.fold_in(stream_key, 6)
    for dim, parts in cuts:
        draws = jnp.exp(jax.random.uniform(jax.random.fold_in(own, dim), (parts,), jnp.float32, low / len(cuts), largest / len(cuts)))
        level = level * jnp.repeat(draws, extent[dim] // parts).reshape([-1 if axis == dim else 1 for axis in range(len(extent))])
    return level


def noise(own_key, extent, width, bound, cuts=(), held_as=jnp.bfloat16):
    result = width * jax.random.normal(own_key, extent, jnp.float32)
    if cuts:
        result = result * levels(own_key, extent, cuts, -0.22, 0.18)
    return jnp.clip(result, -bound, bound).astype(held_as)


def setup_inputs(seed: int = 0) -> dict:
    key_list = jax.random.split(jax.random.key(seed), 3)
    return {
        "panel_rows": noise(key_list[0], (ORDER, K), (K ** -0.25), 0.75, ((0, 4), (1, 8)), jnp.float32),
        "owner_slot": draw_owner_slot(jax.random.fold_in(key_list[2], 71), 0),
    }


def slot_table(owner_slot, group_id, positions, per_group):
    blocks = owner_slot.shape[0]
    block_row = jnp.arange(blocks, dtype=jnp.int32)[:, None]
    block_col = jnp.arange(blocks, dtype=jnp.int32)[None, :]
    inside = (block_row // per_group == group_id) & (block_col <= block_row)
    wanted = jnp.arange(positions, dtype=jnp.int32)[:, None, None]
    matched = inside[None] & (owner_slot[None] == wanted)
    is_live = jnp.any(matched, axis=(1, 2))
    left_block = jnp.sum(jnp.where(matched, block_row[None], 0), axis=(1, 2)).astype(jnp.int32)
    right_block = jnp.sum(jnp.where(matched, block_col[None], 0), axis=(1, 2)).astype(jnp.int32)
    return left_block, right_block, is_live


def reference(panel_rows, owner_slot):
    tiles_all = panel_rows.reshape(NB, BLOCK, K)

    def group_tiles(group_id):
        left_block, right_block, is_live = slot_table(owner_slot, group_id, POS, BR)

        def single(packed_item):
            left_one, right_one, flag = packed_item

            def compute():
                return lax.dot_general(tiles_all[left_one], tiles_all[right_one], (((1,), (1,)), ((), ())),
                                       precision=lax.Precision.HIGHEST, preferred_element_type=jnp.float32)

            def blank():
                return jnp.zeros((BLOCK, BLOCK), jnp.float32)

            return lax.cond(flag, compute, blank)

        return lax.map(single, (left_block, right_block, is_live))

    return lax.map(group_tiles, jnp.arange(N_ROW, dtype=jnp.int32))
```

```python
import functools

import jax
import jax.numpy as jnp
from jax import lax
from jax.experimental import pallas as pl
from jax.experimental.pallas import tpu as pltpu
from jax.sharding import PartitionSpec as P

BLOCK = 512
CHUNK = 256
MESH = pl.DeviceIdType.MESH
NT = (((1,), (1,)), ((), ()))


def slot_table(owner_slot, group_id, positions, per_group):
    blocks = owner_slot.shape[0]
    block_row = jnp.arange(blocks, dtype=jnp.int32)[:, None]
    block_col = jnp.arange(blocks, dtype=jnp.int32)[None, :]
    inside = (block_row // per_group == group_id) & (block_col <= block_row)
    wanted = jnp.arange(positions, dtype=jnp.int32)[:, None, None]
    matched = inside[None] & (owner_slot[None] == wanted)
    is_live = jnp.any(matched, axis=(1, 2))
    left_block = jnp.sum(jnp.where(matched, block_row[None], 0), axis=(1, 2))
    right_block = jnp.sum(jnp.where(matched, block_col[None], 0), axis=(1, 2))
    return (left_block, right_block, is_live)


def kernel(rows_n, cols_n, per_group, slots, table, panel, out, held, ysend, yrecv, zsend, zrecv, own,
           right_hi, right_lo, local_sem, load_recv, load_send, y_send, y_recv, z_send, z_recv):
    row, col = lax.axis_index("row"), lax.axis_index("col")
    chips = rows_n // 2
    far = cols_n // 4
    x, core = row // 2, row % 2
    h, low, y = col // 4, (col // 2) % 2, col % 2
    sibling = (row + 1 - 2 * core, col)
    pair = (row, h * 4 + (1 - low) * 2 + y)
    across = (row, h * 4 + low * 2 + 1 - y)
    beside = [(((x + d) % chips) * 2 + core, col) for d in range(1, chips)]
    ahead = [(row, ((h + d) % far) * 4 + low * 2 + y) for d in range(1, far)]
    partners = [sibling, pair, across] + beside + ahead

    fetch = pltpu.make_async_copy(panel, held.at[pl.ds(row * per_group, per_group), low], local_sem)
    fetch.start()
    barrier = pltpu.get_barrier_semaphore()
    for device in partners:
        pl.semaphore_signal(barrier, inc=1, device_id=device, device_id_type=MESH)
    pl.semaphore_wait(barrier, len(partners))
    fetch.wait()

    sent = []

    def piece(group, side, half):
        return held.at[group * per_group + half, side]

    def push(group, side, half, device):
        copy = pltpu.make_async_remote_copy(
            src_ref=piece(group, side, half),
            dst_ref=piece(group, side, half),
            send_sem=load_send.at[len(sent)],
            recv_sem=load_recv.at[group * per_group + half, side],
            device_id=device,
            device_id_type=MESH,
        )
        copy.start()
        sent.append(copy)

    def arrive(group, side, half):
        pltpu.make_async_remote_copy(
            src_ref=piece(group, side, half),
            dst_ref=piece(group, side, half),
            send_sem=load_send.at[0],
            recv_sem=load_recv.at[group * per_group + half, side],
            device_id=sibling,
            device_id_type=MESH,
        ).wait_recv()

    cut = per_group // 2
    ups, downs = list(range(cut)), list(range(cut, per_group))
    for half in ups + downs:
        for device in beside:
            push(row, low, half, device)
    for half in downs + ups:
        push(row, low, half, pair)
    for half in ups + downs:
        push(row, low, half, sibling)
    others = [((x + chips - d) % chips) * 2 + core for d in range(1, chips)]
    for group in others:
        for half in ups:
            arrive(group, low, half)
            push(group, low, half, pair)
            push(group, low, half, sibling)
    for half in downs:
        arrive(row, 1 - low, half)
        for device in beside:
            push(row, 1 - low, half, device)
        push(row, 1 - low, half, sibling)
    for group in others:
        for half in downs:
            arrive(group, low, half)
            push(group, low, half, sibling)
    for half in ups:
        arrive(row, 1 - low, half)
        push(row, 1 - low, half, sibling)
    for group in others:
        for half in ups + downs:
            arrive(group, 1 - low, half)
            push(group, 1 - low, half, sibling)
    for d in range(chips):
        group = ((x + d) % chips) * 2 + 1 - core
        for side in range(2):
            for half in range(per_group):
                arrive(group, side, half)

    depth = held.shape[-1]

    def tile(position, dst):
        left, right = table[0, position], table[1, position]
        for side in range(2):
            span = pl.ds(side * depth, depth)
            value = held[right, side]
            top = value.astype(jnp.bfloat16)
            right_hi[:, span] = top
            right_lo[:, span] = (value - top.astype(jnp.float32)).astype(jnp.bfloat16)

        @pl.loop(0, BLOCK // CHUNK)
        def _(step):
            rows = pl.ds(pl.multiple_of(step * CHUNK, CHUNK), CHUNK)
            total = jnp.zeros((CHUNK, BLOCK), jnp.float32)
            for side in range(2):
                span = pl.ds(side * depth, depth)
                value = held[left, side, rows, :]
                top = value.astype(jnp.bfloat16)
                rest = (value - top.astype(jnp.float32)).astype(jnp.bfloat16)
                for one, two in ((rest, right_hi), (top, right_lo), (top, right_hi)):
                    total += lax.dot_general(one, two[:, span], NT, preferred_element_type=jnp.float32)
            dst[rows, :] = total

    def place(d, side_y, slot):
        return (((h + d) % far) * 4 + low * 2 + side_y) * slots + slot

    def y_copy(index):
        return pltpu.make_async_remote_copy(
            src_ref=ysend.at[index],
            dst_ref=yrecv.at[index],
            send_sem=y_send.at[index],
            recv_sem=y_recv.at[index],
            device_id=across,
            device_id_type=MESH,
        )

    @pl.loop(0, far * slots)
    def _(index):
        tile(place(index // slots + 1, 1 - y, index % slots), ysend.at[index])
        y_copy(index).start()

    def z_copy(index):
        d = index // slots + 1
        return pltpu.make_async_remote_copy(
            src_ref=zsend.at[index],
            dst_ref=zrecv.at[index],
            send_sem=z_send.at[index],
            recv_sem=z_recv.at[index],
            device_id=(row, ((h + d) % far) * 4 + low * 2 + y),
            device_id_type=MESH,
        )

    hops = (far - 1) * slots

    @pl.loop(0, hops)
    def _(index):
        tile(place(index // slots + 1, y, index % slots), own)
        y_copy(index).wait_recv()
        zsend[index] = own[...] + yrecv[index]
        z_copy(index).start()

    @pl.loop(0, slots)
    def _(slot):
        tile(place(0, y, slot), out.at[slot])

    @pl.loop(0, slots)
    def _(slot):
        y_copy(hops + slot).wait_recv()
        out[slot] = out[slot] + yrecv[hops + slot]

    @pl.loop(0, hops)
    def _(index):
        z_copy(index).wait_recv()
        slot = index % slots
        out[slot] = out[slot] + zrecv[index]

    for slot in range(slots):
        live = table[2, place(0, y, slot)]
        out[slot] = jnp.where(live > 0, out[slot], 0.0)

    for copy in sent:
        copy.wait_send()

    @pl.loop(0, far * slots)
    def _(index):
        y_copy(index).wait_send()

    @pl.loop(0, hops)
    def _(index):
        z_copy(index).wait_send()


def body(panel_rows, owner_slot):
    rows_n = lax.axis_size("row")
    cols_n = lax.axis_size("col")
    slab_rows, depth = panel_rows.shape
    per_group = slab_rows // BLOCK
    blocks = per_group * rows_n
    row_tiles = per_group * (blocks - per_group) + per_group * (per_group + 1) // 2
    slots = (row_tiles + cols_n - 1) // cols_n
    positions = cols_n * slots
    table = jnp.stack([part.astype(jnp.int32) for part in slot_table(owner_slot, lax.axis_index("row"), positions, per_group)])
    chips, far = rows_n // 2, cols_n // 4
    pushes = per_group * ((chips - 1) * 4 + 3) + per_group * (chips - 1)
    tiles = far * slots
    hops = (far - 1) * slots
    summed = pl.pallas_call(
        functools.partial(kernel, rows_n, cols_n, per_group, slots),
        out_shape=jax.ShapeDtypeStruct((slots, BLOCK, BLOCK), jnp.float32),
        in_specs=[pl.BlockSpec(memory_space=pltpu.SMEM), pl.BlockSpec(memory_space=pl.ANY)],
        out_specs=pl.BlockSpec(memory_space=pltpu.VMEM),
        scratch_shapes=[
            pltpu.VMEM((blocks, 2, BLOCK, depth), jnp.float32),
            pltpu.VMEM((tiles, BLOCK, BLOCK), jnp.float32),
            pltpu.VMEM((tiles, BLOCK, BLOCK), jnp.float32),
            pltpu.VMEM((hops, BLOCK, BLOCK), jnp.float32),
            pltpu.VMEM((hops, BLOCK, BLOCK), jnp.float32),
            pltpu.VMEM((BLOCK, BLOCK), jnp.float32),
            pltpu.VMEM((BLOCK, 2 * depth), jnp.bfloat16),
            pltpu.VMEM((BLOCK, 2 * depth), jnp.bfloat16),
            pltpu.SemaphoreType.DMA,
            pltpu.SemaphoreType.DMA((blocks, 2)),
            pltpu.SemaphoreType.DMA((pushes,)),
            pltpu.SemaphoreType.DMA((tiles,)),
            pltpu.SemaphoreType.DMA((tiles,)),
            pltpu.SemaphoreType.DMA((hops,)),
            pltpu.SemaphoreType.DMA((hops,)),
        ],
        compiler_params=pltpu.CompilerParams(
            collective_id=0, has_side_effects=True, vmem_limit_bytes=60 * 2**20
        ),
        cost_estimate=pl.CostEstimate(flops=2 * positions * BLOCK * BLOCK * depth, bytes_accessed=2**22, transcendentals=0),
    )(table, panel_rows.reshape(per_group, BLOCK, depth))
    return summed[None]


def solution(mesh):
    placed = (P("row", "col"), P())
    return jax.shard_map(
        body, mesh=mesh, in_specs=placed, out_specs=P("row", "col", None, None), check_vma=False
    )
```

```python
import functools

import jax
import jax.numpy as jnp
from jax import lax
from jax.experimental import pallas as pl
from jax.experimental.pallas import tpu as pltpu
from jax.sharding import PartitionSpec as P

BLOCK = 512
EDGES = (0, 128, 256, 384, 512)
MESH = pl.DeviceIdType.MESH
NT = (((1,), (1,)), ((), ()))


def slot_table(owner_slot, group_id, positions, per_group):
    blocks = owner_slot.shape[0]
    block_row = jnp.arange(blocks, dtype=jnp.int32)[:, None]
    block_col = jnp.arange(blocks, dtype=jnp.int32)[None, :]
    inside = (block_row // per_group == group_id) & (block_col <= block_row)
    wanted = jnp.arange(positions, dtype=jnp.int32)[:, None, None]
    matched = inside[None] & (owner_slot[None] == wanted)
    is_live = jnp.any(matched, axis=(1, 2))
    left_block = jnp.sum(jnp.where(matched, block_row[None], 0), axis=(1, 2))
    right_block = jnp.sum(jnp.where(matched, block_col[None], 0), axis=(1, 2))
    return (left_block, right_block, is_live)


STAGES = len(EDGES) - 1
PIECES = []
for stage in range(STAGES):
    PIECES.append((stage, EDGES[stage], EDGES[stage + 1], 0, EDGES[stage + 1]))
    if stage:
        PIECES.append((stage, 0, EDGES[stage], EDGES[stage], EDGES[stage + 1]))


def kernel(rows_n, cols_n, per_group, slots, table, panel, out, *scratch):
    count = len(PIECES)
    scratch = list(scratch)

    def take(number):
        taken = scratch[:number]
        del scratch[:number]
        return taken

    held = take(STAGES)
    ysend, yrecv, zsend, zrecv = take(count), take(count), take(count), take(count)
    right_hi, right_lo, local_sem, load_recv, load_send, y_send, y_recv, z_send, z_recv = scratch
    row, col = lax.axis_index("row"), lax.axis_index("col")
    chips = rows_n // 2
    far = cols_n // 4
    x, core = row // 2, row % 2
    h, low, y = col // 4, (col // 2) % 2, col % 2
    sibling = (row + 1 - 2 * core, col)
    pair = (row, h * 4 + (1 - low) * 2 + y)
    across = (row, h * 4 + low * 2 + 1 - y)
    beside = [(((x + d) % chips) * 2 + core, col) for d in range(1, chips)]
    ahead = [(row, ((h + d) % far) * 4 + low * 2 + y) for d in range(1, far)]
    partners = [sibling, pair, across] + beside + ahead

    fetches = []
    for stage in range(STAGES):
        fetch = pltpu.make_async_copy(
            panel.at[:, pl.ds(EDGES[stage], EDGES[stage + 1] - EDGES[stage])],
            held[stage].at[pl.ds(row * per_group, per_group), low],
            local_sem.at[stage],
        )
        fetch.start()
        fetches.append(fetch)
    barrier = pltpu.get_barrier_semaphore()
    for device in partners:
        pl.semaphore_signal(barrier, inc=1, device_id=device, device_id_type=MESH)
    pl.semaphore_wait(barrier, len(partners))

    sent = []

    def push(stage, group, side, half, device):
        block = group * per_group + half
        copy = pltpu.make_async_remote_copy(
            src_ref=held[stage].at[block, side],
            dst_ref=held[stage].at[block, side],
            send_sem=load_send.at[len(sent)],
            recv_sem=load_recv.at[stage, block, side],
            device_id=device,
            device_id_type=MESH,
        )
        copy.start()
        sent.append(copy)

    def arrive(stage, group, side, half):
        block = group * per_group + half
        pltpu.make_async_remote_copy(
            src_ref=held[stage].at[block, side],
            dst_ref=held[stage].at[block, side],
            send_sem=load_send.at[0],
            recv_sem=load_recv.at[stage, block, side],
            device_id=sibling,
            device_id_type=MESH,
        ).wait_recv()

    cut = per_group // 2
    ups, downs = list(range(cut)), list(range(cut, per_group))
    others = [((x + chips - d) % chips) * 2 + core for d in range(1, chips)]

    def first(stage):
        fetches[stage].wait()
        for half in ups + downs:
            for device in beside:
                push(stage, row, low, half, device)
        for half in downs + ups:
            push(stage, row, low, half, pair)
        for half in ups + downs:
            push(stage, row, low, half, sibling)

    def second(stage):
        for group in others:
            for half in ups:
                arrive(stage, group, low, half)
                push(stage, group, low, half, pair)
                push(stage, group, low, half, sibling)
        for half in downs:
            arrive(stage, row, 1 - low, half)
            for device in beside:
                push(stage, row, 1 - low, half, device)
            push(stage, row, 1 - low, half, sibling)

    def third(stage):
        for group in others:
            for half in downs:
                arrive(stage, group, low, half)
                push(stage, group, low, half, sibling)
        for half in ups:
            arrive(stage, row, 1 - low, half)
            push(stage, row, 1 - low, half, sibling)
        for group in others:
            for half in ups + downs:
                arrive(stage, group, 1 - low, half)
                push(stage, group, 1 - low, half, sibling)
        for d in range(chips):
            group = ((x + d) % chips) * 2 + 1 - core
            for side in range(2):
                for half in range(per_group):
                    arrive(stage, group, side, half)

    depth = held[0].shape[-1]

    def split(value):
        top = value.astype(jnp.bfloat16)
        return top, (value - top.astype(jnp.float32)).astype(jnp.bfloat16)

    def strips(stage, position, emit, fresh=0):
        left, right = table[0, position], table[1, position]
        for part in range(fresh, stage + 1):
            for side in range(2):
                where = (slice(EDGES[part], EDGES[part + 1]), slice(side * depth, (side + 1) * depth))
                right_hi[where], right_lo[where] = split(held[part][right, side])

        def product(part, begin, end):
            total = None
            for side in range(2):
                span = slice(side * depth, (side + 1) * depth)
                top, rest = split(held[part][left, side])
                for one, two in ((rest, right_hi), (top, right_lo), (top, right_hi)):
                    term = lax.dot_general(one, two[begin:end, span], NT, preferred_element_type=jnp.float32)
                    total = term if total is None else total + term
            return total

        for number, (own_stage, r0, r1, c0, c1) in enumerate(PIECES):
            if own_stage == stage:
                for part in range(STAGES):
                    if r0 <= EDGES[part] < r1:
                        emit(number, EDGES[part] - r0, EDGES[part + 1] - r0, product(part, c0, c1))

    def numbers(stage):
        return [number for number, piece in enumerate(PIECES) if piece[0] == stage]

    def place(d, side_y, slot):
        return (((h + d) % far) * 4 + low * 2 + side_y) * slots + slot

    def y_copy(number, index):
        return pltpu.make_async_remote_copy(
            src_ref=ysend[number].at[index],
            dst_ref=yrecv[number].at[index],
            send_sem=y_send.at[number, index],
            recv_sem=y_recv.at[number, index],
            device_id=across,
            device_id_type=MESH,
        )

    def z_copy(number, index):
        return pltpu.make_async_remote_copy(
            src_ref=zsend[number].at[index],
            dst_ref=zrecv[number].at[index],
            send_sem=z_send.at[number, index],
            recv_sem=z_recv.at[number, index],
            device_id=(row, ((h + index // slots + 1) % far) * 4 + low * 2 + y),
            device_id_type=MESH,
        )

    tiles, hops = far * slots, (far - 1) * slots

    def y_work(stage):
        @pl.loop(0, tiles)
        def _(index):
            def emit(number, begin, end, value):
                ysend[number][index, begin:end, :] = value

            strips(stage, place(index // slots + 1, 1 - y, index % slots), emit)
            for number in numbers(stage):
                y_copy(number, index).start()

    def z_work(stage):
        @pl.loop(0, hops)
        def _(index):
            def emit(number, begin, end, value):
                zsend[number][index, begin:end, :] = value

            strips(stage, place(index // slots + 1, y, index % slots), emit)
            for number in numbers(stage):
                y_copy(number, index).wait_recv()
                zsend[number][index] += yrecv[number][index]
                z_copy(number, index).start()

    first(0)
    for stage in range(STAGES):
        second(stage)
        if stage + 1 < STAGES:
            first(stage + 1)
        if stage:
            z_work(stage - 1)
        third(stage)
        y_work(stage)
    z_work(STAGES - 1)

    @pl.loop(0, slots)
    def _(slot):
        def emit(number, begin, end, value):
            _, r0, _, c0, c1 = PIECES[number]
            out[slot, r0 + begin:r0 + end, c0:c1] = value

        for stage in range(STAGES):
            strips(stage, place(0, y, slot), emit, stage)
        for number, (_, r0, r1, c0, c1) in enumerate(PIECES):
            y_copy(number, hops + slot).wait_recv()
            out[slot, r0:r1, c0:c1] += yrecv[number][hops + slot]

    for number, (_, r0, r1, c0, c1) in enumerate(PIECES):
        @pl.loop(0, hops)
        def _(index):
            z_copy(number, index).wait_recv()
            slot = index % slots
            out[slot, r0:r1, c0:c1] += zrecv[number][index]

    for slot in range(slots):
        live = table[2, place(0, y, slot)]
        out[slot] = jnp.where(live > 0, out[slot], 0.0)

    for copy in sent:
        copy.wait_send()
    for number in range(count):
        @pl.loop(0, tiles)
        def _(index):
            y_copy(number, index).wait_send()

        @pl.loop(0, hops)
        def _(index):
            z_copy(number, index).wait_send()


def body(panel_rows, owner_slot):
    rows_n = lax.axis_size("row")
    cols_n = lax.axis_size("col")
    slab_rows, depth = panel_rows.shape
    per_group = slab_rows // BLOCK
    blocks = per_group * rows_n
    row_tiles = per_group * (blocks - per_group) + per_group * (per_group + 1) // 2
    slots = (row_tiles + cols_n - 1) // cols_n
    positions = cols_n * slots
    table = jnp.stack([part.astype(jnp.int32) for part in slot_table(owner_slot, lax.axis_index("row"), positions, per_group)])
    chips, far = rows_n // 2, cols_n // 4
    pushes = per_group * ((chips - 1) * 4 + 3) + per_group * (chips - 1)
    tiles = far * slots
    hops = (far - 1) * slots
    summed = pl.pallas_call(
        functools.partial(kernel, rows_n, cols_n, per_group, slots),
        out_shape=jax.ShapeDtypeStruct((slots, BLOCK, BLOCK), jnp.float32),
        in_specs=[pl.BlockSpec(memory_space=pltpu.SMEM), pl.BlockSpec(memory_space=pl.ANY)],
        out_specs=pl.BlockSpec(memory_space=pltpu.VMEM),
        scratch_shapes=[pltpu.VMEM((blocks, 2, EDGES[stage + 1] - EDGES[stage], depth), jnp.float32) for stage in range(STAGES)]
        + [
            pltpu.VMEM((number, r1 - r0, c1 - c0), jnp.float32)
            for number in (tiles, tiles, hops, hops)
            for _, r0, r1, c0, c1 in PIECES
        ]
        + [
            pltpu.VMEM((BLOCK, 2 * depth), jnp.bfloat16),
            pltpu.VMEM((BLOCK, 2 * depth), jnp.bfloat16),
            pltpu.SemaphoreType.DMA((STAGES,)),
            pltpu.SemaphoreType.DMA((STAGES, blocks, 2)),
            pltpu.SemaphoreType.DMA((STAGES * pushes,)),
            pltpu.SemaphoreType.DMA((len(PIECES), tiles)),
            pltpu.SemaphoreType.DMA((len(PIECES), tiles)),
            pltpu.SemaphoreType.DMA((len(PIECES), hops)),
            pltpu.SemaphoreType.DMA((len(PIECES), hops)),
        ],
        compiler_params=pltpu.CompilerParams(
            collective_id=0, has_side_effects=True, vmem_limit_bytes=60 * 2**20
        ),
        cost_estimate=pl.CostEstimate(flops=2 * positions * BLOCK * BLOCK * depth, bytes_accessed=2**22, transcendentals=0),
    )(table, panel_rows.reshape(per_group, BLOCK, depth))
    return summed[None]


def solution(mesh):
    placed = (P("row", "col"), P())
    return jax.shard_map(
        body, mesh=mesh, in_specs=placed, out_specs=P("row", "col", None, None), check_vma=False
    )
```
